32 devices in a mesh: gx: 4 (over z), gy: 4 (over y, x), gz: 2 (over core).
Axes of the slice: x: 2, y: 2, z: 4, core: 2. Of those that a mesh axis runs over, the one named last changes fastest.
Arguments:
- patch_logits: bfloat16 [4, 4, 2, 24, 20736], P('gx', 'gy', 'gz'), may hold values from -12 to 312
- patch_start: int32 [4, 4, 2, 3], replicated, may hold values from 0 to 112, as said below
- patch_owner: int32 [4, 4, 2], replicated, may hold values from 0 to 15, as said below
Outputs:
- probs: float32 [32, 128, 3, 256], P('gx', 'gy', None, 'gz')
The draws below stay inside these ranges and needn't reach their ends.
Inputs may be any that keep to these rules, and one draw needn't show every extreme that they name: `patch_start`: entry [i, j, k, d] is the first cell along dimension d of the patch at lattice position (i, j, k): i * 8 - 8 along x (32 and 128 in place of 8 along y and z), moved by at most 4 cells, then moved inward so that the patch lies inside the volume. `patch_owner`: for every k the entries [:, :, k] are the numbers 0 to 15, each once.
All inputs are finite; a program needn't handle non-finite values.
Results may differ from the reference program's by a relative error of at most 0.0003.
Values may be sent and summed in bfloat16 or wider, within the bound.
A program may use at most 128 MiB of HBM per device.

```python
import jax
import jax.numpy as jnp
from jax import lax

CLASSES = 3
BX = 8
BY = 32
BZ = 128
HALO = 8
JITTER = 4
KX = 4
KY = 4
KZ = 2
NX = 32
NY = 128
NZ = 256
PX = 24
PY = 48
PZ = 144


def draw_patch_logits(key, part):
    full_shape = (KX, KY, KZ, PX, PY, CLASSES, PZ)
    normal_key, spike_key = jax.random.split(jax.random.fold_in(key, 11))
    values = jnp.clip(2.0 * jax.random.normal(normal_key, full_shape, jnp.float32), -12.0, 12.0)
    return values.reshape(KX, KY, KZ, PX, PY * CLASSES * PZ).astype(jnp.bfloat16)


def draw_patch_start(key, part):
    subkeys = jax.random.split(jax.random.fold_in(key, 23), 3)
    counts = (KX, KY, KZ)
    blocks = (BX, BY, BZ)
    extents = (PX, PY, PZ)
    columns = []
    for dimension in range(3):
        lattice = lax.broadcasted_iota(jnp.int32, (KX, KY, KZ), dimension)
        jitter_cells = jax.random.randint(subkeys[dimension], (KX, KY, KZ), -JITTER, JITTER + 1)
        first_cell = lattice * blocks[dimension] - HALO + jitter_cells
        first_cell = jnp.clip(first_cell, 0, counts[dimension] * blocks[dimension] - extents[dimension])
        columns.append(first_cell)
    return jnp.stack(columns, axis=-1).astype(jnp.int32)


def draw_patch_owner(key, part):
    subkeys = jax.random.split(jax.random.fold_in(key, 37), KZ)

    def shuffled(subkey):
        return jax.random.permutation(subkey, KX * KY)
    orders = jax.vmap(shuffled)(subkeys)
    return jnp.transpose(orders).reshape(KX, KY, KZ).astype(jnp.int32)


def setup_inputs(seed: int = 0) -> dict:
    streams_of = jax.random.split(jax.random.key(seed), 4)
    return {
        "patch_logits": draw_patch_logits(jax.random.fold_in(streams_of[3], 71), 0),
        "patch_start": draw_patch_start(jax.random.fold_in(streams_of[3], 71), 0),
        "patch_owner": draw_patch_owner(jax.random.fold_in(streams_of[3], 71), 0),
    }


def profile(length):
    offsets = jnp.arange(length).astype(jnp.float32)
    centre = (length - 1) / 2.0
    spread = length / 4.0
    return jnp.exp(-((offsets - centre) ** 2) / (2.0 * spread * spread))


def reference(patch_logits, patch_start, patch_owner):
    weight = profile(PX)[:, None, None, None] * profile(PY)[None, :, None, None]
    weight = weight * profile(PZ)[None, None, None, :]
    weight_full = jnp.broadcast_to(weight, (PX, PY, 1, PZ))
    totals = jnp.zeros((NX, NY, CLASSES + 1, NZ), jnp.float32)

    def add_patch(flat_index, totals):
        along_x = flat_index // (KY * KZ)
        along_y = (flat_index // KZ) % KY
        along_z = flat_index % KZ
        patch_code = patch_owner[along_x, along_y, along_z]
        home_x = patch_code // KY
        home_y = patch_code % KY
        corner = patch_start[home_x, home_y, along_z].astype(jnp.int32)
        logits = patch_logits[along_x, along_y, along_z].astype(jnp.float32).reshape(PX, PY, CLASSES, PZ)
        contribution = jnp.concatenate([logits * weight, weight_full], axis=2)
        anchor = (corner[0], corner[1], jnp.int32(0), corner[2])
        current = lax.dynamic_slice(totals, anchor, (PX, PY, CLASSES + 1, PZ))
        return lax.dynamic_update_slice(totals, current + contribution, anchor)

    totals = lax.fori_loop(0, KX * KY * KZ, add_patch, totals)
    scores = totals[:, :, :CLASSES] / totals[:, :, CLASSES:]
    return jax.nn.softmax(scores, axis=2)
```

```python
import functools

import jax
import jax.numpy as jnp
from jax import lax
from jax.experimental import pallas as pl
from jax.experimental.pallas import tpu as pltpu
from jax.sharding import PartitionSpec as P

CLASSES = 3
BX = 8
BY = 32
BZ = 128
PX = 24
PY = 48
PZ = 144
RIM = PZ - BZ
STEP = 8
TILES = PX // BX
LINES = PY // STEP
ROWS = BY // STEP
MAIN = LINES * CLASSES
DIFFS = CLASSES - 1
SLOTS = BZ // RIM
SPAN = SLOTS * STEP
GROUP = STEP * CLASSES * PZ
PHASES = BZ // RIM
Y_FIRST = 4
X_FIRST = STEP - Y_FIRST
MESH = pl.DeviceIdType.MESH
F32 = jnp.float32
BF16 = jnp.bfloat16


def profile(offsets, length, keep=True):
    inside = (offsets >= 0) & (offsets < length) & keep
    centre = (length - 1) / 2.0
    spread = length / 4.0
    values = jnp.exp((offsets.astype(F32) - centre) ** 2 * (-0.5 / (spread * spread)))
    return jnp.where(inside, values, 0.0)


def blend_kernel(
    lanes_x, lanes_y, lanes_z,
    start_ref, owner_ref, logits_ref, out_ref,
    raw_ref, cells_ref, move_ref, packed, rim_land, parts, parts_land,
    rows, rows_land, edge_land, sums, sums_land,
    along_ref, plane_ref, rim_plane_ref, row_along_ref, row_plane_ref, edge_plane_ref, weight_ref,
    raw_in, cells_out, cells_in, rims_out, rims_in, parts_out, parts_in,
    rows_out, rows_in, edges_out, edges_in, sums_out, sums_in,
    *land,
):
    place_x = lax.axis_index("gx")
    place_y = lax.axis_index("gy")
    place_z = lax.axis_index("gz")
    sides = (1,) if lanes_z == 2 else (1, lanes_z - 1)
    cells_y = lanes_y * BY

    def ahead(place, d, size):
        return lax.rem(place + d, size)

    def corner_of(code, layer):
        return [start_ref[code // lanes_y, k, layer, lax.rem(code, lanes_y)] for k in range(3)]

    def settle(ref, sem):
        pltpu.make_async_copy(ref, ref, sem).wait()

    barrier = pltpu.get_barrier_semaphore()
    peers = [{"gz": ahead(place_z, s, lanes_z)} for s in sides]
    for axis, place, size in (("gx", place_x, lanes_x), ("gy", place_y, lanes_y)):
        for d in range(1, size):
            there = {axis: ahead(place, d, size)}
            peers.append(there)
            peers += [{**there, "gz": ahead(place_z, s, lanes_z)} for s in sides]
    for peer in peers:
        pl.semaphore_signal(barrier, inc=1, device_id=peer, device_id_type=MESH)

    groups = PY // STEP
    loads = []
    for g in range(groups):
        lanes = pl.ds(g * GROUP, GROUP)
        loads.append(pltpu.make_async_copy(logits_ref.at[:, lanes], raw_ref.at[:, lanes], raw_in.at[g]))
        loads[-1].start()

    code = owner_ref[place_x, place_z, place_y]
    start_x, start_y, start_z = corner_of(code, place_z)
    shift_z = place_z * BZ - start_z

    k = lax.broadcasted_iota(jnp.int32, (2 * BZ, 2 * BZ), 0)
    n = lax.broadcasted_iota(jnp.int32, (2 * BZ, 2 * BZ), 1)
    edge = lax.rem(n, RIM) + shift_z
    edge = edge + jnp.where(edge < RIM, BZ, -RIM)
    ahead_by = k - jnp.where(n < BZ, n + shift_z, edge)
    for m in range(PHASES):
        move_ref[m] = jnp.where(ahead_by == m * RIM, 1.0, 0.0).astype(BF16)

    r = lax.broadcasted_iota(jnp.int32, (PX, PX), 0)
    p = lax.broadcasted_iota(jnp.int32, (PX, PX), 1) + lax.rem(start_x, PX)
    pick = jnp.where(jnp.where(p >= PX, p - PX, p) == r, 1.0, 0.0).astype(BF16)
    for g in range(groups):
        lanes = slice(g * GROUP, (g + 1) * GROUP)
        loads[g].wait()
        cells = jnp.dot(pick, raw_ref[:, lanes], preferred_element_type=F32)
        cells = cells.astype(BF16)
        for i in range(GROUP // BZ):
            cells_ref[g * (GROUP // BZ) + i] = cells[:, i * BZ : (i + 1) * BZ]

    lane = lax.broadcasted_iota(jnp.int32, (BX, BZ), 1)
    sub = lax.broadcasted_iota(jnp.int32, (BX, BZ), 0)
    slot_of_lane = lane // RIM

    def line_of(y, y0):
        return jnp.clip(lax.shift_right_arithmetic(y - y0, 3), 0, LINES - 1)

    def pack(r):
        phase = lax.rem(r - start_y + cells_y, STEP)
        first = (start_y + phase) // STEP
        for c in range(CLASSES):
            at = phase * (STEP * CLASSES + CLASSES) + c * (STEP + 1)
            block = at // PHASES
            halves = []
            for half in range(2):
                lines = [cells_ref[u * (GROUP // BZ) + block + half] for u in range(LINES)]
                halves.append(jnp.concatenate(lines, axis=0))
            moved = jnp.dot(
                jnp.concatenate(halves, axis=1), move_ref[lax.rem(at, PHASES)], preferred_element_type=F32
            )
            rims = [jnp.zeros((BX, BZ), F32)] * TILES
            for u in range(LINES):
                here = slot_of_lane == lax.rem(first + u, SLOTS)
                for j in range(TILES):
                    cells = slice(u * PX + j * BX, u * PX + (j + 1) * BX)
                    packed[r, j, u * CLASSES + c] = moved[cells, :BZ].astype(BF16)
                    rims[j] = jnp.where(here, moved[cells, BZ:], rims[j])
            for j in range(TILES):
                packed[r, j, MAIN + c] = rims[j].astype(BF16)

    def cut_rows(k):
        for b in range(lanes_y):
            for t in range(ROWS):
                at = line_of(b * BY + t * STEP + k, start_y) * CLASSES
                for j in range(TILES):
                    for c in range(CLASSES):
                        rows[k, b, j, t * CLASSES + c] = packed[k, j, at + c]

    far_x = sorted(range(1, lanes_x), key=lambda d: -min(d, lanes_x - d))
    far_y = sorted(range(1, lanes_y), key=lambda d: -min(d, lanes_y - d))

    def remote(src, dst, send, recv, where):
        pltpu.make_async_remote_copy(
            src_ref=src, dst_ref=dst, send_sem=send, recv_sem=recv, device_id=where, device_id_type=MESH
        ).start()

    def send_x(k):
        r = Y_FIRST + k
        for d in far_x + [0]:
            there = ahead(place_x, d, lanes_x)
            tile = lax.rem(there, TILES)
            if d:
                cells = packed.at[r, tile, pl.ds(0, MAIN)]
                remote(cells, land[k].at[d], cells_out.at[k], cells_in.at[k], {"gx": there})
            rims = packed.at[r, tile, pl.ds(MAIN, CLASSES)]
            for s, step in enumerate(sides):
                where = {"gx": there, "gz": ahead(place_z, step, lanes_z)}
                remote(rims, rim_land.at[k, s, d], rims_out.at[k], rims_in.at[k], where)

    def send_y(k):
        for d in far_y + [0]:
            there = ahead(place_y, d, lanes_y)
            if d:
                remote(rows.at[k, there], rows_land.at[k, d], rows_out.at[k], rows_in.at[k], {"gy": there})
            rims = packed.at[k, pl.ds(0, TILES), pl.ds(MAIN, CLASSES)]
            for s, step in enumerate(sides):
                where = {"gy": there, "gz": ahead(place_z, step, lanes_z)}
                remote(rims, edge_land.at[k, s, d], edges_out.at[k], edges_in.at[k], where)

    for k in range(max(X_FIRST, Y_FIRST)):
        if k < Y_FIRST:
            pack(k)
            cut_rows(k)
            if k == 0:
                pl.semaphore_wait(barrier, len(peers))
            send_y(k)
        if k < X_FIRST:
            pack(Y_FIRST + k)
            if k == 0 and not Y_FIRST:
                pl.semaphore_wait(barrier, len(peers))
            send_x(k)

    cell_x = place_x * BX + sub
    cell_z = place_z * BZ + lane
    row = lax.broadcasted_iota(jnp.int32, (cells_y, BZ), 0)
    cell_y = place_y * BY + lax.broadcasted_iota(jnp.int32, (BY, BZ), 0)
    low = [place_z > 0 if lanes_z == 2 else step == 1 for step in sides]
    layers = [place_z + jnp.where(side, -1, 1) for side in low]
    kept = [jnp.clip(layer, 0, lanes_z - 1) for layer in layers]
    rim_z = [place_z * BZ + lax.rem(lane, RIM) + jnp.where(side, 0, BZ - RIM) for side in low]

    starts_y = []
    rim_starts_y = {}
    for d in range(lanes_x):
        source = lax.rem(place_x - d + lanes_x, lanes_x)
        x0, y0, z0 = corner_of(owner_ref[source, place_z, place_y], place_z)
        starts_y.append(y0)
        plane_ref[d] = profile(cell_x - x0, PX) * profile(cell_z - z0, PZ)
        along_ref[d] = profile(row - y0, PY)
        for s, layer in enumerate(layers):
            x0, y0, z0 = corner_of(owner_ref[source, kept[s], place_y], kept[s])
            rim_starts_y[s, d] = y0
            rim_plane_ref[s, d] = profile(cell_x - x0, PX) * profile(rim_z[s] - z0, PZ, layer == kept[s])
    edge_starts_y = {}
    for d in range(lanes_y):
        source = lax.rem(place_y - d + lanes_y, lanes_y)
        x0, y0, z0 = corner_of(owner_ref[place_x, place_z, source], place_z)
        row_along_ref[d] = profile(cell_y - y0, PY)
        along_z = profile(cell_z - z0, PZ)
        for b in range(lanes_x):
            row_plane_ref[d, b] = profile(b * BX + sub - x0, PX) * along_z
        for s, layer in enumerate(layers):
            x0, y0, z0 = corner_of(owner_ref[place_x, kept[s], source], kept[s])
            edge_starts_y[s, d] = y0
            along_z = profile(rim_z[s] - z0, PZ, layer == kept[s])
            for b in range(lanes_x):
                edge_plane_ref[s, d, b] = profile(b * BX + sub - x0, PX) * along_z

    def weigh(code, carry):
        for step in (0, 1) if lanes_z == 2 else (-1, 0, 1):
            reach = step if lanes_z == 2 else place_z + step
            layer = jnp.clip(reach, 0, lanes_z - 1)
            x0, y0, z0 = corner_of(code, layer)
            along = profile(cell_y - y0, PY)
            plane = profile(cell_x - x0, PX) * profile(cell_z - z0, PZ, layer == reach)
            for y in range(BY):
                weight_ref[y] = weight_ref[y] + plane * along[y : y + 1]
        return carry

    weight_ref[...] = jnp.zeros(weight_ref.shape, F32)
    lax.fori_loop(0, lanes_x * lanes_y, weigh, 0)
    for y in range(BY):
        weight_ref[y] = 1.0 / weight_ref[y]

    spans = -(-cells_y // SPAN)
    rim_lane = [jnp.where(side, lane, BZ - 1 - lane) < RIM for side in low]

    def blend_x(k):
        r = Y_FIRST + k
        settle(land[k].at[pl.ds(1, lanes_x - 1)], cells_in.at[k])
        settle(rim_land.at[k], rims_in.at[k])
        rims = {}
        for s in range(len(sides)):
            for d in range(lanes_x):
                cells = [rim_land[k, s, d, c].astype(F32) for c in range(CLASSES)]
                for span in range(spans):
                    y = span * SPAN + slot_of_lane * STEP + r
                    weight = rim_plane_ref[s, d] * profile(y - rim_starts_y[s, d], PY)
                    for e in range(DIFFS):
                        term = (cells[e + 1] - cells[0]) * weight
                        rims[s, span, e] = rims[s, span, e] + term if d else term
            for span in range(spans):
                for e in range(DIFFS):
                    total = rims[s, span, e]
                    rims[s, span, e] = jnp.where(low[s], total, pltpu.roll(total, BZ - RIM, 1))
        for b in range(lanes_y):
            for t in range(ROWS):
                y = b * BY + t * STEP + r
                slot = (b * ROWS + t) % SLOTS
                totals = []
                for e in range(DIFFS):
                    total = 0.0
                    for s in range(len(sides)):
                        rim = rims[s, b * BY // SPAN, e]
                        rim = pltpu.roll(rim, BZ - slot * RIM, 1) if slot else rim
                        total = jnp.where(rim_lane[s], rim, total)
                    totals.append(total)
                for d in range(lanes_x):
                    at = line_of(y, starts_y[d]) * CLASSES
                    if d:
                        cells = [land[k][d, at + c].astype(F32) for c in range(CLASSES)]
                    else:
                        tile = lax.rem(place_x, TILES)
                        cells = [packed[r, tile, at + c].astype(F32) for c in range(CLASSES)]
                    weight = plane_ref[d] * along_ref[d, pl.ds(y, 1)]
                    for e in range(DIFFS):
                        totals[e] = totals[e] + (cells[e + 1] - cells[0]) * weight
                for e in range(DIFFS):
                    parts[k, b, t, e] = totals[e]
        for d in far_y:
            there = ahead(place_y, d, lanes_y)
            remote(parts.at[k, there], parts_land.at[k, d], parts_out.at[k], parts_in.at[k], {"gy": there})

    def blend_y(k):
        settle(rows_land.at[k, pl.ds(1, lanes_y - 1)], rows_in.at[k])
        settle(edge_land.at[k], edges_in.at[k])
        first = lax.rem(place_y * ROWS, SLOTS)
        rims = {}
        for s in range(len(sides)):
            for d in range(lanes_y):
                y = (place_y * ROWS - first + slot_of_lane) * STEP + k
                along = profile(y - edge_starts_y[s, d], PY)
                for j in range(min(TILES, lanes_x)):
                    cells = [edge_land[k, s, d, j, c].astype(F32) for c in range(CLASSES)]
                    terms = [(cells[e + 1] - cells[0]) * along for e in range(DIFFS)]
                    for b in range(j, lanes_x, TILES):
                        for e in range(DIFFS):
                            term = terms[e] * edge_plane_ref[s, d, b]
                            rims[s, b, e] = rims[s, b, e] + term if d else term
        turn = [lax.rem(2 * BZ - first * RIM - jnp.where(side, 0, RIM), BZ) for side in low]
        rims = {at: pltpu.roll(total, turn[at[0]], 1) for at, total in rims.items()}
        for j in range(min(TILES, lanes_x)):
            for t in range(ROWS):
                y = t * STEP + k
                totals = {}
                for b in range(j, lanes_x, TILES):
                    for e in range(DIFFS):
                        total = 0.0
                        for s in range(len(sides)):
                            rim = pltpu.roll(rims[s, b, e], BZ - t * RIM, 1) if t else rims[s, b, e]
                            total = jnp.where(rim_lane[s], rim, total)
                        totals[b, e] = total
                for d in range(lanes_y):
                    if d:
                        cells = [rows_land[k, d, j, t * CLASSES + c].astype(F32) for c in range(CLASSES)]
                    else:
                        cells = [rows[k, place_y, j, t * CLASSES + c].astype(F32) for c in range(CLASSES)]
                    along = row_along_ref[d, pl.ds(y, 1)]
                    terms = [(cells[e + 1] - cells[0]) * along for e in range(DIFFS)]
                    for b in range(j, lanes_x, TILES):
                        for e in range(DIFFS):
                            totals[b, e] = totals[b, e] + terms[e] * row_plane_ref[d, b]
                for (b, e), total in totals.items():
                    sums[k, b, t, e] = total
        hop(0, k)

    def take(k, way, b):
        settle(sums_land.at[k, way, b], sums_in.at[k, way, b])
        for t in range(ROWS):
            for e in range(DIFFS):
                sums[k, b, t, e] = sums[k, b, t, e] + sums_land[k, way, b, t, e]

    def hop(h, k):
        for way in range(2):
            @pl.when(place_x == (lanes_x - 1 - h if way else h))
            def _():
                past = range(lanes_x - 1 - h) if way else range(lanes_x - 1, h, -1)
                there = place_x - 1 if way else place_x + 1
                for b in past:
                    if h:
                        take(k, way, b)
                    remote(
                        sums.at[k, b], sums_land.at[k, way, b], sums_out.at[k], sums_in.at[k, way, b], {"gx": there}
                    )

    def write(y, totals):
        scores = [total * weight_ref[y] for total in totals]
        top = jnp.maximum(functools.reduce(jnp.maximum, scores), 0.0)
        powers = [jnp.exp(-top)] + [jnp.exp(s - top) for s in scores]
        norm = 1.0 / functools.reduce(jnp.add, powers)
        for c in range(CLASSES):
            out_ref[y, c] = powers[c] * norm

    def finish_x(k):
        settle(parts_land.at[k, pl.ds(1, lanes_y - 1)], parts_in.at[k])
        for t in range(ROWS):
            totals = []
            for e in range(DIFFS):
                total = parts[k, place_y, t, e]
                for d in far_y:
                    total = total + parts_land[k, d, t, e]
                totals.append(total)
            write(t * STEP + Y_FIRST + k, totals)

    def finish_y(k):
        @pl.when(place_x > 0)
        def _():
            take(k, 0, place_x)

        @pl.when(place_x < lanes_x - 1)
        def _():
            take(k, 1, place_x)

        for t in range(ROWS):
            write(t * STEP + k, [sums[k, place_x, t, e] for e in range(DIFFS)])

    for i in range(max(X_FIRST, Y_FIRST) + lanes_x):
        if i < Y_FIRST:
            blend_y(i)
        if i < X_FIRST:
            blend_x(i)
        for h in range(1, lanes_x - 1):
            if 0 <= i - h + 1 < Y_FIRST:
                hop(h, i - h + 1)
        if 0 <= i - 1 < X_FIRST:
            finish_x(i - 1)
        if 0 <= i - lanes_x + 2 < Y_FIRST:
            finish_y(i - lanes_x + 2)

    for k in range(X_FIRST):
        settle(land[k].at[pl.ds(1, lanes_x - 1)], cells_out.at[k])
        settle(rim_land.at[k], rims_out.at[k])
        settle(parts_land.at[k, pl.ds(1, lanes_y - 1)], parts_out.at[k])
    for k in range(Y_FIRST):
        settle(rows_land.at[k, pl.ds(1, lanes_y - 1)], rows_out.at[k])
        settle(edge_land.at[k], edges_out.at[k])
        settle(sums.at[k, pl.ds(0, lanes_x - 1)], sums_out.at[k])


VMEM = pl.BlockSpec(memory_space=pltpu.VMEM)
SMEM = pl.BlockSpec(memory_space=pltpu.SMEM)


def per_device(patch_logits, patch_start, patch_owner):
    lanes_x = lax.axis_size("gx")
    lanes_y = lax.axis_size("gy")
    lanes_z = lax.axis_size("gz")
    sides = 1 if lanes_z == 2 else 2
    lines = PY * CLASSES * PZ
    dma = pltpu.SemaphoreType.DMA
    probs = pl.pallas_call(
        functools.partial(blend_kernel, lanes_x, lanes_y, lanes_z),
        out_shape=pltpu.VMEM((BY, CLASSES, BX, BZ), F32),
        in_specs=[SMEM, SMEM, pl.BlockSpec(memory_space=pl.ANY)],
        out_specs=VMEM,
        scratch_shapes=[
            pltpu.VMEM((PX, lines), BF16),
            pltpu.VMEM((lines // BZ, PX, BZ), BF16),
            pltpu.VMEM((PHASES, 2 * BZ, 2 * BZ), BF16),
            pltpu.VMEM((STEP, TILES, MAIN + CLASSES, BX, BZ), BF16),
            pltpu.VMEM((X_FIRST, sides, lanes_x, CLASSES, BX, BZ), BF16),
            pltpu.VMEM((X_FIRST, lanes_y, ROWS, DIFFS, BX, BZ), F32),
            pltpu.VMEM((X_FIRST, lanes_y, ROWS, DIFFS, BX, BZ), F32),
            pltpu.VMEM((Y_FIRST, lanes_y, TILES, ROWS * CLASSES, BX, BZ), BF16),
            pltpu.VMEM((Y_FIRST, lanes_y, TILES, ROWS * CLASSES, BX, BZ), BF16),
            pltpu.VMEM((Y_FIRST, sides, lanes_y, TILES, CLASSES, BX, BZ), BF16),
            pltpu.VMEM((Y_FIRST, lanes_x, ROWS, DIFFS, BX, BZ), F32),
            pltpu.VMEM((Y_FIRST, 2, lanes_x, ROWS, DIFFS, BX, BZ), F32),
            pltpu.VMEM((lanes_x, lanes_y * BY, BZ), F32),
            pltpu.VMEM((lanes_x, BX, BZ), F32),
            pltpu.VMEM((sides, lanes_x, BX, BZ), F32),
            pltpu.VMEM((lanes_y, BY, BZ), F32),
            pltpu.VMEM((lanes_y, lanes_x, BX, BZ), F32),
            pltpu.VMEM((sides, lanes_y, lanes_x, BX, BZ), F32),
            pltpu.VMEM((BY, BX, BZ), F32),
            dma((PY // STEP,)),
            *[dma((X_FIRST,))] * 6,
            *[dma((Y_FIRST,))] * 5,
            dma((Y_FIRST, 2, lanes_x)),
            *[pltpu.VMEM((lanes_x, MAIN, BX, BZ), BF16)] * X_FIRST,
        ],
        compiler_params=pltpu.CompilerParams(collective_id=0, has_side_effects=True),
    )(
        jnp.transpose(patch_start, (0, 3, 2, 1)),
        jnp.transpose(patch_owner, (0, 2, 1)),
        patch_logits[0, 0, 0],
    )
    return jnp.transpose(probs, (2, 0, 1, 3))


def solution(mesh):
    return jax.shard_map(
        per_device,
        mesh=mesh,
        in_specs=(P("gx", "gy", "gz", None, None), P(), P()),
        out_specs=P("gx", "gy", None, "gz"),
        check_vma=False,
    )
```

```python
import functools

import jax
import jax.numpy as jnp
from jax import lax
from jax.experimental import pallas as pl
from jax.experimental.pallas import tpu as pltpu
from jax.sharding import PartitionSpec as P

CLASSES = 3
BX = 8
BY = 32
BZ = 128
PX = 24
PY = 48
PZ = 144
RIM = PZ - BZ
STEP = 8
TILES = PX // BX
LINES = PY // STEP
ROWS = BY // STEP
MAIN = LINES * CLASSES
DIFFS = CLASSES - 1
SLOTS = BZ // RIM
SPAN = SLOTS * STEP
GROUP = STEP * CLASSES * PZ
PHASES = BZ // RIM
Y_FIRST = 4
X_FIRST = STEP - Y_FIRST
AHEAD = 2
MESH = pl.DeviceIdType.MESH
F32 = jnp.float32
BF16 = jnp.bfloat16


def profile(offsets, length, keep=True):
    inside = (offsets >= 0) & (offsets < length) & keep
    centre = (length - 1) / 2.0
    spread = length / 4.0
    values = jnp.exp((offsets.astype(F32) - centre) ** 2 * (-0.5 / (spread * spread)))
    return jnp.where(inside, values, 0.0)


def events(send_x, blend_y, blend_x, join_y, cross_x, finish_x, finish_y):
    return [
        (blend_y, 0), (blend_x, 0), (blend_y, 1), (blend_y, 2), (join_y, 0), (send_x, 2), (blend_x, 1),
        (blend_y, 3), (finish_x, 0), (join_y, 1), (send_x, 3), (cross_x, 0), (join_y, 2), (finish_x, 1), (blend_x, 2),
        (cross_x, 1), (finish_y, 0), (join_y, 3), (cross_x, 2), (finish_y, 1), (blend_x, 3), (cross_x, 3),
        (finish_x, 2), (finish_y, 2), (finish_x, 3), (finish_y, 3),
    ]


def blend_kernel(
    lanes_x, lanes_y, lanes_z,
    starts_ref, owners_ref, logits_ref, out_ref,
    start_ref, owner_ref, raw_ref, cells_ref, move_ref, packed, rim_land, parts, parts_land,
    rows, rows_land, edge_land, sums, halves, halves_land, pair_land, cross_land,
    along_ref, plane_ref, rim_plane_ref, row_along_ref, row_plane_ref, edge_plane_ref, weight_ref,
    table_in, raw_in, cells_out, cells_in, rims_out, rims_in, parts_out, parts_in,
    rows_out, rows_in, edges_out, edges_in, halves_out, halves_in, pair_out, pair_in, cross_out, cross_in,
    *land,
):
    place_x = lax.axis_index("gx")
    place_y = lax.axis_index("gy")
    place_z = lax.axis_index("gz")
    sides = (1,) if lanes_z == 2 else (1, lanes_z - 1)
    cells_y = lanes_y * BY

    def ahead(place, d, size):
        return lax.rem(place + d, size)

    def corner_of(code, layer):
        return [start_ref[code // lanes_y, k, layer, lax.rem(code, lanes_y)] for k in range(3)]

    def settle(ref, sem):
        pltpu.make_async_copy(ref, ref, sem).wait()

    side_y = lax.rem(place_y, 2)
    next_y = place_y + 1 - 2 * side_y
    same_y = [lax.rem(place_y + 2 * o, lanes_y) for o in range(lanes_y // 2)]
    side_x = lax.rem(place_x, 2)
    pair_x = place_x // 2
    tables = [
        pltpu.make_async_copy(starts_ref, start_ref, table_in.at[0]),
        pltpu.make_async_copy(owners_ref, owner_ref, table_in.at[1]),
    ]
    for table in tables:
        table.start()
    barrier = pltpu.get_barrier_semaphore()
    near = [{"gx": ahead(place_x, d, lanes_x)} for d in range(1, lanes_x)]
    peers = near + [{"gy": ahead(place_y, d, lanes_y)} for d in range(1, lanes_y)]
    for there in near + [{}, {"gy": next_y}]:
        peers += [{**there, "gz": ahead(place_z, s, lanes_z)} for s in sides]
    for peer in peers:
        pl.semaphore_signal(barrier, inc=1, device_id=peer, device_id_type=MESH)

    groups = PY // STEP
    loads = []
    for g in range(groups):
        lanes = pl.ds(g * GROUP, GROUP)
        loads.append(pltpu.make_async_copy(logits_ref.at[:, lanes], raw_ref.at[:, lanes], raw_in.at[g]))
        loads[-1].start()

    for table in tables:
        table.wait()
    code = owner_ref[place_x, place_z, place_y]
    start_x, start_y, start_z = corner_of(code, place_z)
    shift_z = place_z * BZ - start_z

    k = lax.broadcasted_iota(jnp.int32, (2 * BZ, 2 * BZ), 0)
    n = lax.broadcasted_iota(jnp.int32, (2 * BZ, 2 * BZ), 1)
    edge = lax.rem(n, RIM) + shift_z
    edge = edge + jnp.where(edge < RIM, BZ, -RIM)
    ahead_by = k - jnp.where(n < BZ, n + shift_z, edge)
    for m in range(PHASES):
        move_ref[m] = jnp.where(ahead_by == m * RIM, 1.0, 0.0).astype(BF16)

    r = lax.broadcasted_iota(jnp.int32, (PX, PX), 0)
    p = lax.broadcasted_iota(jnp.int32, (PX, PX), 1) + lax.rem(start_x, PX)
    pick = jnp.where(jnp.where(p >= PX, p - PX, p) == r, 1.0, 0.0).astype(BF16)
    for g in range(groups):
        lanes = slice(g * GROUP, (g + 1) * GROUP)
        loads[g].wait()
        cells = jnp.dot(pick, raw_ref[:, lanes], preferred_element_type=F32)
        cells = cells.astype(BF16)
        for i in range(GROUP // BZ):
            cells_ref[g * (GROUP // BZ) + i] = cells[:, i * BZ : (i + 1) * BZ]

    lane = lax.broadcasted_iota(jnp.int32, (BX, BZ), 1)
    sub = lax.broadcasted_iota(jnp.int32, (BX, BZ), 0)
    slot_of_lane = lane // RIM

    def line_of(y, y0):
        return jnp.clip(lax.shift_right_arithmetic(y - y0, 3), 0, LINES - 1)

    def pack(r):
        phase = lax.rem(r - start_y + cells_y, STEP)
        first = (start_y + phase) // STEP
        for c in range(CLASSES):
            at = phase * (STEP * CLASSES + CLASSES) + c * (STEP + 1)
            block = at // PHASES
            halves = []
            for half in range(2):
                lines = [cells_ref[u * (GROUP // BZ) + block + half] for u in range(LINES)]
                halves.append(jnp.concatenate(lines, axis=0))
            moved = jnp.dot(
                jnp.concatenate(halves, axis=1), move_ref[lax.rem(at, PHASES)], preferred_element_type=F32
            )
            rims = [jnp.zeros((BX, BZ), F32)] * TILES
            for u in range(LINES):
                here = slot_of_lane == lax.rem(first + u, SLOTS)
                for j in range(TILES):
                    cells = slice(u * PX + j * BX, u * PX + (j + 1) * BX)
                    packed[r, j, u * CLASSES + c] = moved[cells, :BZ].astype(BF16)
                    rims[j] = jnp.where(here, moved[cells, BZ:], rims[j])
            for j in range(TILES):
                packed[r, j, MAIN + c] = rims[j].astype(BF16)

    def cut_rows(k):
        for q in range(2):
            for t in range(ROWS):
                line = lax.shift_right_arithmetic(q * BY + t * STEP + k - start_y, 3)
                for b in range(q + 2, lanes_y, 2):
                    other = lax.shift_right_arithmetic(b * BY + t * STEP + k - start_y, 3)
                    line = jnp.where((other >= 0) & (other < LINES), other, line)
                at = jnp.clip(line, 0, LINES - 1) * CLASSES
                for j in range(TILES):
                    for c in range(CLASSES):
                        rows[k, q, j, t * CLASSES + c] = packed[k, j, at + c]

    far_x = sorted(range(1, lanes_x), key=lambda d: -min(d, lanes_x - d))
    far_y = sorted(range(1, lanes_y), key=lambda d: -min(d, lanes_y - d))

    def remote(src, dst, send, recv, where):
        pltpu.make_async_remote_copy(
            src_ref=src, dst_ref=dst, send_sem=send, recv_sem=recv, device_id=where, device_id_type=MESH
        ).start()

    def send_x(k):
        r = Y_FIRST + k
        for d in far_x + [0]:
            there = ahead(place_x, d, lanes_x)
            tile = lax.rem(there, TILES)
            if d:
                cells = packed.at[r, tile, pl.ds(0, MAIN)]
                remote(cells, land[k].at[d], cells_out.at[k], cells_in.at[k], {"gx": there})
            rims = packed.at[r, tile, pl.ds(MAIN, CLASSES)]
            for s, step in enumerate(sides):
                where = {"gx": there, "gz": ahead(place_z, step, lanes_z)}
                remote(rims, rim_land.at[k, s, d], rims_out.at[k], rims_in.at[k], where)

    def send_y(k):
        remote(rows.at[k, 1 - side_y], rows_land.at[k], rows_out.at[k], rows_in.at[k], {"gy": next_y})
        rims = packed.at[k, pl.ds(0, TILES), pl.ds(MAIN, CLASSES)]
        for s, step in enumerate(sides):
            for d, there in enumerate(({}, {"gy": next_y})):
                where = {**there, "gz": ahead(place_z, step, lanes_z)}
                remote(rims, edge_land.at[k, s, d], edges_out.at[k], edges_in.at[k], where)

    for k in range(max(X_FIRST, Y_FIRST)):
        if k < Y_FIRST:
            pack(k)
            cut_rows(k)
            if k == 0:
                pl.semaphore_wait(barrier, len(peers))
            send_y(k)
        if k < X_FIRST:
            pack(Y_FIRST + k)
            if k == 0 and not Y_FIRST:
                pl.semaphore_wait(barrier, len(peers))
            if k < AHEAD:
                send_x(k)

    cell_x = place_x * BX + sub
    cell_z = place_z * BZ + lane
    row = lax.broadcasted_iota(jnp.int32, (cells_y, BZ), 0)
    cell_y = place_y * BY + lax.broadcasted_iota(jnp.int32, (BY, BZ), 0)
    low = [place_z > 0 if lanes_z == 2 else step == 1 for step in sides]
    layers = [place_z + jnp.where(side, -1, 1) for side in low]
    kept = [jnp.clip(layer, 0, lanes_z - 1) for layer in layers]
    rim_z = [place_z * BZ + lax.rem(lane, RIM) + jnp.where(side, 0, BZ - RIM) for side in low]

    starts_y = []
    rim_starts_y = {}
    for d in range(lanes_x):
        source = lax.rem(place_x - d + lanes_x, lanes_x)
        x0, y0, z0 = corner_of(owner_ref[source, place_z, place_y], place_z)
        starts_y.append(y0)
        plane_ref[d] = profile(cell_x - x0, PX) * profile(cell_z - z0, PZ)
        along_ref[d] = profile(row - y0, PY)
        for s, layer in enumerate(layers):
            x0, y0, z0 = corner_of(owner_ref[source, kept[s], place_y], kept[s])
            rim_starts_y[s, d] = y0
            rim_plane_ref[s, d] = profile(cell_x - x0, PX) * profile(rim_z[s] - z0, PZ, layer == kept[s])
    edge_starts_y = {}
    for d, source in enumerate((place_y, next_y)):
        x0, y0, z0 = corner_of(owner_ref[place_x, place_z, source], place_z)
        for o, b in enumerate(same_y):
            row_along_ref[o, d] = profile((b - place_y) * BY + cell_y - y0, PY)
        along_z = profile(cell_z - z0, PZ)
        for b in range(lanes_x):
            row_plane_ref[d, b] = profile(b * BX + sub - x0, PX) * along_z
        for s, layer in enumerate(layers):
            x0, y0, z0 = corner_of(owner_ref[place_x, kept[s], source], kept[s])
            edge_starts_y[s, d] = y0
            along_z = profile(rim_z[s] - z0, PZ, layer == kept[s])
            for b in range(lanes_x):
                edge_plane_ref[s, d, b] = profile(b * BX + sub - x0, PX) * along_z

    def weigh(code, carry):
        for step in (0, 1) if lanes_z == 2 else (-1, 0, 1):
            reach = step if lanes_z == 2 else place_z + step
            layer = jnp.clip(reach, 0, lanes_z - 1)
            x0, y0, z0 = corner_of(code, layer)
            along = profile(cell_y - y0, PY)
            plane = profile(cell_x - x0, PX) * profile(cell_z - z0, PZ, layer == reach)
            for y in range(BY):
                weight_ref[y] = weight_ref[y] + plane * along[y : y + 1]
        return carry

    weight_ref[...] = jnp.zeros(weight_ref.shape, F32)
    lax.fori_loop(0, lanes_x * lanes_y, weigh, 0)
    for y in range(BY):
        weight_ref[y] = 1.0 / weight_ref[y]

    spans = -(-cells_y // SPAN)
    rim_lane = [jnp.where(side, lane, BZ - 1 - lane) < RIM for side in low]

    def blend_x(k):
        r = Y_FIRST + k
        settle(land[k].at[pl.ds(1, lanes_x - 1)], cells_in.at[k])
        settle(rim_land.at[k], rims_in.at[k])
        rims = {}
        for s in range(len(sides)):
            for d in range(lanes_x):
                cells = [rim_land[k, s, d, c].astype(F32) for c in range(CLASSES)]
                for span in range(spans):
                    y = span * SPAN + slot_of_lane * STEP + r
                    weight = rim_plane_ref[s, d] * profile(y - rim_starts_y[s, d], PY)
                    for e in range(DIFFS):
                        term = (cells[e + 1] - cells[0]) * weight
                        rims[s, span, e] = rims[s, span, e] + term if d else term
            for span in range(spans):
                for e in range(DIFFS):
                    total = rims[s, span, e]
                    rims[s, span, e] = jnp.where(low[s], total, pltpu.roll(total, BZ - RIM, 1))
        for b in range(lanes_y):
            for t in range(ROWS):
                y = b * BY + t * STEP + r
                slot = (b * ROWS + t) % SLOTS
                totals = []
                for e in range(DIFFS):
                    total = 0.0
                    for s in range(len(sides)):
                        rim = rims[s, b * BY // SPAN, e]
                        rim = pltpu.roll(rim, BZ - slot * RIM, 1) if slot else rim
                        total = jnp.where(rim_lane[s], rim, total)
                    totals.append(total)
                for d in range(lanes_x):
                    at = line_of(y, starts_y[d]) * CLASSES
                    if d:
                        cells = [land[k][d, at + c].astype(F32) for c in range(CLASSES)]
                    else:
                        tile = lax.rem(place_x, TILES)
                        cells = [packed[r, tile, at + c].astype(F32) for c in range(CLASSES)]
                    weight = plane_ref[d] * along_ref[d, pl.ds(y, 1)]
                    for e in range(DIFFS):
                        totals[e] = totals[e] + (cells[e + 1] - cells[0]) * weight
                for e in range(DIFFS):
                    parts[k, b, t, e] = totals[e]
        for d in far_y:
            there = ahead(place_y, d, lanes_y)
            remote(parts.at[k, there], parts_land.at[k, d], parts_out.at[k], parts_in.at[k], {"gy": there})

    def blend_y(k):
        settle(rows_land.at[k], rows_in.at[k])
        settle(edge_land.at[k], edges_in.at[k])
        first = lax.rem(place_y * ROWS, SLOTS)
        rims = {}
        for s in range(len(sides)):
            for d in range(2):
                along = []
                for b in same_y:
                    y = (b * ROWS - first + slot_of_lane) * STEP + k
                    along.append(profile(y - edge_starts_y[s, d], PY))
                for j in range(min(TILES, lanes_x)):
                    cells = [edge_land[k, s, d, j, c].astype(F32) for c in range(CLASSES)]
                    for o in range(len(same_y)):
                        terms = [(cells[e + 1] - cells[0]) * along[o] for e in range(DIFFS)]
                        for b in range(j, lanes_x, TILES):
                            for e in range(DIFFS):
                                term = terms[e] * edge_plane_ref[s, d, b]
                                rims[s, o, b, e] = rims[s, o, b, e] + term if d else term
        turn = [lax.rem(2 * BZ - first * RIM - jnp.where(side, 0, RIM), BZ) for side in low]
        rims = {at: pltpu.roll(total, turn[at[0]], 1) for at, total in rims.items()}
        for j in range(min(TILES, lanes_x)):
            for t in range(ROWS):
                y = t * STEP + k
                totals = {}
                for o in range(len(same_y)):
                    for b in range(j, lanes_x, TILES):
                        for e in range(DIFFS):
                            total = 0.0
                            for s in range(len(sides)):
                                rim = rims[s, o, b, e]
                                rim = pltpu.roll(rim, BZ - t * RIM, 1) if t else rim
                                total = jnp.where(rim_lane[s], rim, total)
                            totals[o, b, e] = total
                for d in range(2):
                    if d:
                        cells = [rows_land[k, j, t * CLASSES + c].astype(F32) for c in range(CLASSES)]
                    else:
                        cells = [rows[k, side_y, j, t * CLASSES + c].astype(F32) for c in range(CLASSES)]
                    for o in range(len(same_y)):
                        along = row_along_ref[o, d, pl.ds(y, 1)]
                        terms = [(cells[e + 1] - cells[0]) * along for e in range(DIFFS)]
                        for b in range(j, lanes_x, TILES):
                            for e in range(DIFFS):
                                totals[o, b, e] = totals[o, b, e] + terms[e] * row_plane_ref[d, b]
                for (o, b, e), total in totals.items():
                    if o:
                        halves[k, o - 1, b, t, e] = total
                    else:
                        sums[k, b, t, e] = total
        for o in range(1, len(same_y)):
            remote(
                halves.at[k, o - 1], halves_land.at[k, o - 1], halves_out.at[k], halves_in.at[k], {"gy": same_y[o]}
            )

    def add(k, b, other):
        for t in range(ROWS):
            for e in range(DIFFS):
                sums[k, b, t, e] = sums[k, b, t, e] + other[t, e]

    def join_y(k):
        settle(halves_land.at[k], halves_in.at[k])
        for o in range(1, len(same_y)):
            for b in range(lanes_x):
                add(k, b, halves_land.at[k, o - 1, b])
        for side in range(2):
            for b in range(lanes_x) if side else range(lanes_x - 1, -1, -1):
                @pl.when((side_x == side) & (b < place_x if side else b > place_x))
                def _():
                    there = place_x + 1 - 2 * side
                    remote(sums.at[k, b], pair_land.at[k, b], pair_out.at[k], pair_in.at[k, b], {"gx": there})

    def cross_x(k):
        for side in range(2):
            for b in range(lanes_x - 1, -1, -1) if side else range(lanes_x):
                @pl.when((side_x == side) & (b > place_x if side else b < place_x))
                def _():
                    settle(pair_land.at[k, b], pair_in.at[k, b])
                    add(k, b, pair_land.at[k, b])
                    remote(
                        sums.at[k, b], cross_land.at[k, pair_x], cross_out.at[k], cross_in.at[k, pair_x], {"gx": b}
                    )

    def write(y, totals):
        scores = [total * weight_ref[y] for total in totals]
        top = jnp.maximum(functools.reduce(jnp.maximum, scores), 0.0)
        powers = [jnp.exp(-top)] + [jnp.exp(s - top) for s in scores]
        norm = 1.0 / functools.reduce(jnp.add, powers)
        for c in range(CLASSES):
            out_ref[y, c] = powers[c] * norm

    def finish_x(k):
        settle(parts_land.at[k, pl.ds(1, lanes_y - 1)], parts_in.at[k])
        for t in range(ROWS):
            totals = []
            for e in range(DIFFS):
                total = parts[k, place_y, t, e]
                for d in far_y:
                    total = total + parts_land[k, d, t, e]
                totals.append(total)
            write(t * STEP + Y_FIRST + k, totals)

    def finish_y(k):
        settle(pair_land.at[k, place_x], pair_in.at[k, place_x])
        others = [pair_land.at[k, place_x]]
        for o in range(1, lanes_x // 2):
            g = lax.rem(pair_x + o, lanes_x // 2)
            settle(cross_land.at[k, g], cross_in.at[k, g])
            others.append(cross_land.at[k, g])
        for t in range(ROWS):
            totals = []
            for e in range(DIFFS):
                total = sums[k, place_x, t, e]
                for other in others:
                    total = total + other[t, e]
                totals.append(total)
            write(t * STEP + k, totals)

    for event, k in events(send_x, blend_y, blend_x, join_y, cross_x, finish_x, finish_y):
        event(k)

    for k in range(X_FIRST):
        settle(land[k].at[pl.ds(1, lanes_x - 1)], cells_out.at[k])
        settle(rim_land.at[k], rims_out.at[k])
        settle(parts_land.at[k, pl.ds(1, lanes_y - 1)], parts_out.at[k])
    for k in range(Y_FIRST):
        settle(rows_land.at[k], rows_out.at[k])
        settle(edge_land.at[k], edges_out.at[k])
        settle(halves_land.at[k], halves_out.at[k])
    for x in range(lanes_x):
        @pl.when(place_x == x)
        def _():
            paired = x if x % 2 else lanes_x - 1 - x
            crossed = lanes_x - 1 - paired
            for k in range(Y_FIRST):
                settle(sums.at[k, pl.ds(0, paired)], pair_out.at[k])
                if crossed:
                    settle(sums.at[k, pl.ds(0, crossed)], cross_out.at[k])


VMEM = pl.BlockSpec(memory_space=pltpu.VMEM)


def per_device(patch_logits, patch_start, patch_owner):
    lanes_x = lax.axis_size("gx")
    lanes_y = lax.axis_size("gy")
    lanes_z = lax.axis_size("gz")
    sides = 1 if lanes_z == 2 else 2
    lines = PY * CLASSES * PZ
    dma = pltpu.SemaphoreType.DMA
    probs = pl.pallas_call(
        functools.partial(blend_kernel, lanes_x, lanes_y, lanes_z),
        out_shape=pltpu.VMEM((BY, CLASSES, BX, BZ), F32),
        in_specs=[pl.BlockSpec(memory_space=pl.ANY)] * 3,
        out_specs=VMEM,
        scratch_shapes=[
            pltpu.SMEM((lanes_x, 3, lanes_z, lanes_y), jnp.int32),
            pltpu.SMEM((lanes_x, lanes_z, lanes_y), jnp.int32),
            pltpu.VMEM((PX, lines), BF16),
            pltpu.VMEM((lines // BZ, PX, BZ), BF16),
            pltpu.VMEM((PHASES, 2 * BZ, 2 * BZ), BF16),
            pltpu.VMEM((STEP, TILES, MAIN + CLASSES, BX, BZ), BF16),
            pltpu.VMEM((X_FIRST, sides, lanes_x, CLASSES, BX, BZ), BF16),
            pltpu.VMEM((X_FIRST, lanes_y, ROWS, DIFFS, BX, BZ), F32),
            pltpu.VMEM((X_FIRST, lanes_y, ROWS, DIFFS, BX, BZ), F32),
            pltpu.VMEM((Y_FIRST, 2, TILES, ROWS * CLASSES, BX, BZ), BF16),
            pltpu.VMEM((Y_FIRST, TILES, ROWS * CLASSES, BX, BZ), BF16),
            pltpu.VMEM((Y_FIRST, sides, 2, TILES, CLASSES, BX, BZ), BF16),
            pltpu.VMEM((Y_FIRST, lanes_x, ROWS, DIFFS, BX, BZ), F32),
            pltpu.VMEM((Y_FIRST, lanes_y // 2 - 1, lanes_x, ROWS, DIFFS, BX, BZ), F32),
            pltpu.VMEM((Y_FIRST, lanes_y // 2 - 1, lanes_x, ROWS, DIFFS, BX, BZ), F32),
            pltpu.VMEM((Y_FIRST, lanes_x, ROWS, DIFFS, BX, BZ), F32),
            pltpu.VMEM((Y_FIRST, lanes_x // 2, ROWS, DIFFS, BX, BZ), F32),
            pltpu.VMEM((lanes_x, lanes_y * BY, BZ), F32),
            pltpu.VMEM((lanes_x, BX, BZ), F32),
            pltpu.VMEM((sides, lanes_x, BX, BZ), F32),
            pltpu.VMEM((lanes_y // 2, 2, BY, BZ), F32),
            pltpu.VMEM((2, lanes_x, BX, BZ), F32),
            pltpu.VMEM((sides, 2, lanes_x, BX, BZ), F32),
            pltpu.VMEM((BY, BX, BZ), F32),
            dma((2,)),
            dma((PY // STEP,)),
            *[dma((X_FIRST,))] * 6,
            *[dma((Y_FIRST,))] * 7,
            dma((Y_FIRST, lanes_x)),
            dma((Y_FIRST,)),
            dma((Y_FIRST, lanes_x // 2)),
            *[pltpu.VMEM((lanes_x, MAIN, BX, BZ), BF16)] * X_FIRST,
        ],
        compiler_params=pltpu.CompilerParams(collective_id=0, has_side_effects=True),
    )(
        jnp.transpose(patch_start, (0, 3, 2, 1)),
        jnp.transpose(patch_owner, (0, 2, 1)),
        patch_logits[0, 0, 0],
    )
    return jnp.transpose(probs, (2, 0, 1, 3))


def solution(mesh):
    return jax.shard_map(
        per_device,
        mesh=mesh,
        in_specs=(P("gx", "gy", "gz", None, None), P(), P()),
        out_specs=P("gx", "gy", None, "gz"),
        check_vma=False,
    )
```

```python
import functools

import jax
import jax.numpy as jnp
from jax import lax
from jax.experimental import pallas as pl
from jax.experimental.pallas import tpu as pltpu
from jax.sharding import PartitionSpec as P

CLASSES = 3
BX = 8
BY = 32
BZ = 128
PX = 24
PY = 48
PZ = 144
RIM = PZ - BZ
STEP = 8
TILES = PX // BX
LINES = PY // STEP
ROWS = BY // STEP
MAIN = LINES * CLASSES
DIFFS = CLASSES - 1
SLOTS = BZ // RIM
SPAN = SLOTS * STEP
GROUP = STEP * CLASSES * PZ
PHASES = BZ // RIM
Y_FIRST = 3
X_FIRST = STEP - Y_FIRST
EARLY = ((0, 1), (0, 1), (0,), (), (),)
MESH = pl.DeviceIdType.MESH
F32 = jnp.float32
BF16 = jnp.bfloat16


def profile(offsets, length, keep=True):
    inside = (offsets >= 0) & (offsets < length) & keep
    centre = (length - 1) / 2.0
    spread = length / 4.0
    values = jnp.exp((offsets.astype(F32) - centre) ** 2 * (-0.5 / (spread * spread)))
    return jnp.where(inside, values, 0.0)


def blend_kernel(
    lanes_x, lanes_y, lanes_z,
    starts_ref, owners_ref, logits_ref, out_ref,
    start_ref, owner_ref, raw_ref, cells_ref, move_ref, packed, rim_land, parts, parts_land,
    rows, rows_land, edge_land, sums, pair_land, cross_land,
    along_ref, plane_ref, rim_plane_ref, row_along_ref, row_plane_ref, edge_plane_ref, weight_ref,
    table_in, raw_in, cells_out, cells_in, rims_out, rims_in, parts_out, parts_in,
    rows_out, rows_in, edges_out, edges_in, pair_out, pair_in, cross_out, cross_in,
    *land,
):
    place_x = lax.axis_index("gx")
    place_y = lax.axis_index("gy")
    place_z = lax.axis_index("gz")
    sides = (1,) if lanes_z == 2 else (1, lanes_z - 1)
    cells_y = lanes_y * BY

    def ahead(place, d, size):
        return lax.rem(place + d, size)

    def corner_of(code, layer):
        return [start_ref[code // lanes_y, k, layer, lax.rem(code, lanes_y)] for k in range(3)]

    def settle(ref, sem):
        pltpu.make_async_copy(ref, ref, sem).wait()

    side_x = lax.rem(place_x, 2)
    pair_x = place_x // 2
    tables = [
        pltpu.make_async_copy(starts_ref, start_ref, table_in.at[0]),
        pltpu.make_async_copy(owners_ref, owner_ref, table_in.at[1]),
    ]
    for table in tables:
        table.start()
    barrier = pltpu.get_barrier_semaphore()
    near = [{"gx": ahead(place_x, d, lanes_x)} for d in range(1, lanes_x)]
    near += [{"gy": ahead(place_y, d, lanes_y)} for d in range(1, lanes_y)]
    peers = list(near)
    for there in near + [{}]:
        peers += [{**there, "gz": ahead(place_z, s, lanes_z)} for s in sides]
    for peer in peers:
        pl.semaphore_signal(barrier, inc=1, device_id=peer, device_id_type=MESH)

    groups = PY // STEP
    loads = []
    for g in range(groups):
        lanes = pl.ds(g * GROUP, GROUP)
        loads.append(pltpu.make_async_copy(logits_ref.at[:, lanes], raw_ref.at[:, lanes], raw_in.at[g]))
        loads[-1].start()

    for table in tables:
        table.wait()
    code = owner_ref[place_x, place_z, place_y]
    start_x, start_y, start_z = corner_of(code, place_z)
    shift_z = place_z * BZ - start_z

    k = lax.broadcasted_iota(jnp.int32, (2 * BZ, 2 * BZ), 0)
    n = lax.broadcasted_iota(jnp.int32, (2 * BZ, 2 * BZ), 1)
    edge = lax.rem(n, RIM) + shift_z
    edge = edge + jnp.where(edge < RIM, BZ, -RIM)
    ahead_by = k - jnp.where(n < BZ, n + shift_z, edge)
    for m in range(PHASES):
        move_ref[m] = jnp.where(ahead_by == m * RIM, 1.0, 0.0).astype(BF16)

    r = lax.broadcasted_iota(jnp.int32, (PX, PX), 0)
    p = lax.broadcasted_iota(jnp.int32, (PX, PX), 1) + lax.rem(start_x, PX)
    pick = jnp.where(jnp.where(p >= PX, p - PX, p) == r, 1.0, 0.0).astype(BF16)
    for g in range(groups):
        lanes = slice(g * GROUP, (g + 1) * GROUP)
        loads[g].wait()
        cells = jnp.dot(pick, raw_ref[:, lanes], preferred_element_type=F32)
        cells = cells.astype(BF16)
        for i in range(GROUP // BZ):
            cells_ref[g * (GROUP // BZ) + i] = cells[:, i * BZ : (i + 1) * BZ]

    lane = lax.broadcasted_iota(jnp.int32, (BX, BZ), 1)
    sub = lax.broadcasted_iota(jnp.int32, (BX, BZ), 0)
    slot_of_lane = lane // RIM

    def line_of(y, y0):
        return jnp.clip(lax.shift_right_arithmetic(y - y0, 3), 0, LINES - 1)

    def pack(r):
        phase = lax.rem(r - start_y + cells_y, STEP)
        first = (start_y + phase) // STEP
        for c in range(CLASSES):
            at = phase * (STEP * CLASSES + CLASSES) + c * (STEP + 1)
            block = at // PHASES
            halves = []
            for half in range(2):
                lines = [cells_ref[u * (GROUP // BZ) + block + half] for u in range(LINES)]
                halves.append(jnp.concatenate(lines, axis=0))
            moved = jnp.dot(
                jnp.concatenate(halves, axis=1), move_ref[lax.rem(at, PHASES)], preferred_element_type=F32
            )
            rims = [jnp.zeros((BX, BZ), F32)] * TILES
            for u in range(LINES):
                here = slot_of_lane == lax.rem(first + u, SLOTS)
                for j in range(TILES):
                    cells = slice(u * PX + j * BX, u * PX + (j + 1) * BX)
                    packed[r, j, u * CLASSES + c] = moved[cells, :BZ].astype(BF16)
                    rims[j] = jnp.where(here, moved[cells, BZ:], rims[j])
            for j in range(TILES):
                packed[r, j, MAIN + c] = rims[j].astype(BF16)

    def cut_rows(k):
        for b in range(lanes_y):
            for t in range(ROWS):
                at = line_of(b * BY + t * STEP + k, start_y) * CLASSES
                for j in range(TILES):
                    for c in range(CLASSES):
                        rows[k, b, j, t * CLASSES + c] = packed[k, j, at + c]

    far_x = sorted(range(1, lanes_x), key=lambda d: -min(d, lanes_x - d))
    far_y = sorted(range(1, lanes_y), key=lambda d: -min(d, lanes_y - d))

    def remote(src, dst, send, recv, where):
        pltpu.make_async_remote_copy(
            src_ref=src, dst_ref=dst, send_sem=send, recv_sem=recv, device_id=where, device_id_type=MESH
        ).start()

    middle = jnp.where((place_x > 0) & (place_x < lanes_x - 1), 1, 0)

    def send_x(k, side):
        r = Y_FIRST + k

        @pl.when(middle == side)
        def _():
            for d in far_x + [0]:
                there = ahead(place_x, d, lanes_x)
                tile = lax.rem(there, TILES)
                if d:
                    cells = packed.at[r, tile, pl.ds(0, MAIN)]
                    remote(cells, land[k].at[d], cells_out.at[k], cells_in.at[k], {"gx": there})
                rims = packed.at[r, tile, pl.ds(MAIN, CLASSES)]
                for s, step in enumerate(sides):
                    where = {"gx": there, "gz": ahead(place_z, step, lanes_z)}
                    remote(rims, rim_land.at[k, s, d], rims_out.at[k], rims_in.at[k], where)

    def send_y(k):
        for d in far_y + [0]:
            there = ahead(place_y, d, lanes_y)
            if d:
                remote(rows.at[k, there], rows_land.at[k, d], rows_out.at[k], rows_in.at[k], {"gy": there})
            rims = packed.at[k, pl.ds(0, TILES), pl.ds(MAIN, CLASSES)]
            for s, step in enumerate(sides):
                where = {"gy": there, "gz": ahead(place_z, step, lanes_z)}
                remote(rims, edge_land.at[k, s, d], edges_out.at[k], edges_in.at[k], where)

    for k in range(max(X_FIRST, Y_FIRST)):
        if k < Y_FIRST:
            pack(k)
            cut_rows(k)
            if k == 0:
                pl.semaphore_wait(barrier, len(peers))
            send_y(k)
        if k < X_FIRST:
            pack(Y_FIRST + k)
            if k == 0 and not Y_FIRST:
                pl.semaphore_wait(barrier, len(peers))
            for side in EARLY[k]:
                send_x(k, side)

    cell_x = place_x * BX + sub
    cell_z = place_z * BZ + lane
    row = lax.broadcasted_iota(jnp.int32, (cells_y, BZ), 0)
    cell_y = place_y * BY + lax.broadcasted_iota(jnp.int32, (BY, BZ), 0)
    low = [place_z > 0 if lanes_z == 2 else step == 1 for step in sides]
    layers = [place_z + jnp.where(side, -1, 1) for side in low]
    kept = [jnp.clip(layer, 0, lanes_z - 1) for layer in layers]
    rim_z = [place_z * BZ + lax.rem(lane, RIM) + jnp.where(side, 0, BZ - RIM) for side in low]

    starts_y = []
    rim_starts_y = {}
    for d in range(lanes_x):
        source = lax.rem(place_x - d + lanes_x, lanes_x)
        x0, y0, z0 = corner_of(owner_ref[source, place_z, place_y], place_z)
        starts_y.append(y0)
        plane_ref[d] = profile(cell_x - x0, PX) * profile(cell_z - z0, PZ)
        along_ref[d] = profile(row - y0, PY)
        for s, layer in enumerate(layers):
            x0, y0, z0 = corner_of(owner_ref[source, kept[s], place_y], kept[s])
            rim_starts_y[s, d] = y0
            rim_plane_ref[s, d] = profile(cell_x - x0, PX) * profile(rim_z[s] - z0, PZ, layer == kept[s])
    edge_starts_y = {}
    for d in range(lanes_y):
        source = lax.rem(place_y - d + lanes_y, lanes_y)
        x0, y0, z0 = corner_of(owner_ref[place_x, place_z, source], place_z)
        row_along_ref[d] = profile(cell_y - y0, PY)
        along_z = profile(cell_z - z0, PZ)
        for b in range(lanes_x):
            row_plane_ref[d, b] = profile(b * BX + sub - x0, PX) * along_z
        for s, layer in enumerate(layers):
            x0, y0, z0 = corner_of(owner_ref[place_x, kept[s], source], kept[s])
            edge_starts_y[s, d] = y0
            along_z = profile(rim_z[s] - z0, PZ, layer == kept[s])
            for b in range(lanes_x):
                edge_plane_ref[s, d, b] = profile(b * BX + sub - x0, PX) * along_z

    def weigh(code, carry):
        for step in (0, 1) if lanes_z == 2 else (-1, 0, 1):
            reach = step if lanes_z == 2 else place_z + step
            layer = jnp.clip(reach, 0, lanes_z - 1)
            x0, y0, z0 = corner_of(code, layer)
            along = profile(cell_y - y0, PY)
            plane = profile(cell_x - x0, PX) * profile(cell_z - z0, PZ, layer == reach)
            for y in range(BY):
                weight_ref[y] = weight_ref[y] + plane * along[y : y + 1]
        return carry

    weight_ref[...] = jnp.zeros(weight_ref.shape, F32)
    lax.fori_loop(0, lanes_x * lanes_y, weigh, 0)
    for y in range(BY):
        weight_ref[y] = 1.0 / weight_ref[y]

    spans = -(-cells_y // SPAN)
    rim_lane = [jnp.where(side, lane, BZ - 1 - lane) < RIM for side in low]

    def blend_x(k):
        r = Y_FIRST + k
        settle(land[k].at[pl.ds(1, lanes_x - 1)], cells_in.at[k])
        settle(rim_land.at[k], rims_in.at[k])
        rims = {}
        for s in range(len(sides)):
            for d in range(lanes_x):
                cells = [rim_land[k, s, d, c].astype(F32) for c in range(CLASSES)]
                for span in range(spans):
                    y = span * SPAN + slot_of_lane * STEP + r
                    weight = rim_plane_ref[s, d] * profile(y - rim_starts_y[s, d], PY)
                    for e in range(DIFFS):
                        term = (cells[e + 1] - cells[0]) * weight
                        rims[s, span, e] = rims[s, span, e] + term if d else term
            for span in range(spans):
                for e in range(DIFFS):
                    total = rims[s, span, e]
                    rims[s, span, e] = jnp.where(low[s], total, pltpu.roll(total, BZ - RIM, 1))
        for b in range(lanes_y):
            for t in range(ROWS):
                y = b * BY + t * STEP + r
                slot = (b * ROWS + t) % SLOTS
                totals = []
                for e in range(DIFFS):
                    total = 0.0
                    for s in range(len(sides)):
                        rim = rims[s, b * BY // SPAN, e]
                        rim = pltpu.roll(rim, BZ - slot * RIM, 1) if slot else rim
                        total = jnp.where(rim_lane[s], rim, total)
                    totals.append(total)
                for d in range(lanes_x):
                    at = line_of(y, starts_y[d]) * CLASSES
                    if d:
                        cells = [land[k][d, at + c].astype(F32) for c in range(CLASSES)]
                    else:
                        tile = lax.rem(place_x, TILES)
                        cells = [packed[r, tile, at + c].astype(F32) for c in range(CLASSES)]
                    weight = plane_ref[d] * along_ref[d, pl.ds(y, 1)]
                    for e in range(DIFFS):
                        totals[e] = totals[e] + (cells[e + 1] - cells[0]) * weight
                for e in range(DIFFS):
                    parts[k, b, t, e] = totals[e]
        for d in far_y:
            there = ahead(place_y, d, lanes_y)
            remote(parts.at[k, there], parts_land.at[k, d], parts_out.at[k], parts_in.at[k], {"gy": there})

    def blend_y(k):
        settle(rows_land.at[k, pl.ds(1, lanes_y - 1)], rows_in.at[k])
        settle(edge_land.at[k], edges_in.at[k])
        first = lax.rem(place_y * ROWS, SLOTS)
        rims = {}
        for s in range(len(sides)):
            for d in range(lanes_y):
                y = (place_y * ROWS - first + slot_of_lane) * STEP + k
                along = profile(y - edge_starts_y[s, d], PY)
                for j in range(min(TILES, lanes_x)):
                    cells = [edge_land[k, s, d, j, c].astype(F32) for c in range(CLASSES)]
                    terms = [(cells[e + 1] - cells[0]) * along for e in range(DIFFS)]
                    for b in range(j, lanes_x, TILES):
                        for e in range(DIFFS):
                            term = terms[e] * edge_plane_ref[s, d, b]
                            rims[s, b, e] = rims[s, b, e] + term if d else term
        turn = [lax.rem(2 * BZ - first * RIM - jnp.where(side, 0, RIM), BZ) for side in low]
        rims = {at: pltpu.roll(total, turn[at[0]], 1) for at, total in rims.items()}
        for j in range(min(TILES, lanes_x)):
            for t in range(ROWS):
                y = t * STEP + k
                totals = {}
                for b in range(j, lanes_x, TILES):
                    for e in range(DIFFS):
                        total = 0.0
                        for s in range(len(sides)):
                            rim = pltpu.roll(rims[s, b, e], BZ - t * RIM, 1) if t else rims[s, b, e]
                            total = jnp.where(rim_lane[s], rim, total)
                        totals[b, e] = total
                for d in range(lanes_y):
                    if d:
                        cells = [rows_land[k, d, j, t * CLASSES + c].astype(F32) for c in range(CLASSES)]
                    else:
                        cells = [rows[k, place_y, j, t * CLASSES + c].astype(F32) for c in range(CLASSES)]
                    along = row_along_ref[d, pl.ds(y, 1)]
                    terms = [(cells[e + 1] - cells[0]) * along for e in range(DIFFS)]
                    for b in range(j, lanes_x, TILES):
                        for e in range(DIFFS):
                            totals[b, e] = totals[b, e] + terms[e] * row_plane_ref[d, b]
                for (b, e), total in totals.items():
                    sums[k, b, t, e] = total
        pair_up(k)

    def add(k, b, other):
        for t in range(ROWS):
            for e in range(DIFFS):
                sums[k, b, t, e] = sums[k, b, t, e] + other[t, e]

    def pair_up(k):
        for side in range(2):
            for b in range(lanes_x) if side else range(lanes_x - 1, -1, -1):
                @pl.when((side_x == side) & (b < place_x if side else b > place_x))
                def _():
                    there = place_x + 1 - 2 * side
                    remote(sums.at[k, b], pair_land.at[k, b], pair_out.at[k], pair_in.at[k, b], {"gx": there})

    def cross_x(k):
        for side in range(2):
            for b in range(lanes_x - 1, -1, -1) if side else range(lanes_x):
                @pl.when((side_x == side) & (b > place_x if side else b < place_x))
                def _():
                    settle(pair_land.at[k, b], pair_in.at[k, b])
                    add(k, b, pair_land.at[k, b])
                    remote(
                        sums.at[k, b], cross_land.at[k, pair_x], cross_out.at[k], cross_in.at[k, pair_x], {"gx": b}
                    )

    def write(y, totals):
        scores = [total * weight_ref[y] for total in totals]
        top = jnp.maximum(functools.reduce(jnp.maximum, scores), 0.0)
        powers = [jnp.exp(-top)] + [jnp.exp(s - top) for s in scores]
        norm = 1.0 / functools.reduce(jnp.add, powers)
        for c in range(CLASSES):
            out_ref[y, c] = powers[c] * norm

    def finish_x(k):
        settle(parts_land.at[k, pl.ds(1, lanes_y - 1)], parts_in.at[k])
        for t in range(ROWS):
            totals = []
            for e in range(DIFFS):
                total = parts[k, place_y, t, e]
                for d in far_y:
                    total = total + parts_land[k, d, t, e]
                totals.append(total)
            write(t * STEP + Y_FIRST + k, totals)

    def finish_y(k):
        settle(pair_land.at[k, place_x], pair_in.at[k, place_x])
        others = [pair_land.at[k, place_x]]
        for o in range(1, lanes_x // 2):
            g = lax.rem(pair_x + o, lanes_x // 2)
            settle(cross_land.at[k, g], cross_in.at[k, g])
            others.append(cross_land.at[k, g])
        for t in range(ROWS):
            totals = []
            for e in range(DIFFS):
                total = sums[k, place_x, t, e]
                for other in others:
                    total = total + other[t, e]
                totals.append(total)
            write(t * STEP + k, totals)

    for event, *which in [
        (blend_y, 0),
        (blend_x, 0),
        (send_x, 2, 1),
        (send_x, 3, 0),
        (cross_x, 0),
        (blend_y, 1),
        (blend_x, 1),
        (send_x, 4, 0),
        (send_x, 3, 1),
        (cross_x, 1),
        (finish_x, 0),
        (blend_y, 2),
        (blend_x, 2),
        (send_x, 4, 1),
        (finish_y, 0),
        (cross_x, 2),
        (finish_x, 1),
        (blend_x, 3),
        (finish_y, 1),
        (finish_x, 2),
        (blend_x, 4),
        (finish_y, 2),
        (finish_x, 3),
        (finish_x, 4),
    ]:
        event(*which)

    for k in range(X_FIRST):
        settle(land[k].at[pl.ds(1, lanes_x - 1)], cells_out.at[k])
        settle(rim_land.at[k], rims_out.at[k])
        settle(parts_land.at[k, pl.ds(1, lanes_y - 1)], parts_out.at[k])
    for k in range(Y_FIRST):
        settle(rows_land.at[k, pl.ds(1, lanes_y - 1)], rows_out.at[k])
        settle(edge_land.at[k], edges_out.at[k])
    for x in range(lanes_x):
        @pl.when(place_x == x)
        def _():
            paired = x if x % 2 else lanes_x - 1 - x
            crossed = lanes_x - 1 - paired
            for k in range(Y_FIRST):
                settle(sums.at[k, pl.ds(0, paired)], pair_out.at[k])
                if crossed:
                    settle(sums.at[k, pl.ds(0, crossed)], cross_out.at[k])


VMEM = pl.BlockSpec(memory_space=pltpu.VMEM)


def per_device(patch_logits, patch_start, patch_owner):
    lanes_x = lax.axis_size("gx")
    lanes_y = lax.axis_size("gy")
    lanes_z = lax.axis_size("gz")
    sides = 1 if lanes_z == 2 else 2
    lines = PY * CLASSES * PZ
    dma = pltpu.SemaphoreType.DMA
    probs = pl.pallas_call(
        functools.partial(blend_kernel, lanes_x, lanes_y, lanes_z),
        out_shape=pltpu.VMEM((BY, CLASSES, BX, BZ), F32),
        in_specs=[pl.BlockSpec(memory_space=pl.ANY)] * 3,
        out_specs=VMEM,
        scratch_shapes=[
            pltpu.SMEM((lanes_x, 3, lanes_z, lanes_y), jnp.int32),
            pltpu.SMEM((lanes_x, lanes_z, lanes_y), jnp.int32),
            pltpu.VMEM((PX, lines), BF16),
            pltpu.VMEM((lines // BZ, PX, BZ), BF16),
            pltpu.VMEM((PHASES, 2 * BZ, 2 * BZ), BF16),
            pltpu.VMEM((STEP, TILES, MAIN + CLASSES, BX, BZ), BF16),
            pltpu.VMEM((X_FIRST, sides, lanes_x, CLASSES, BX, BZ), BF16),
            pltpu.VMEM((X_FIRST, lanes_y, ROWS, DIFFS, BX, BZ), F32),
            pltpu.VMEM((X_FIRST, lanes_y, ROWS, DIFFS, BX, BZ), F32),
            pltpu.VMEM((Y_FIRST, lanes_y, TILES, ROWS * CLASSES, BX, BZ), BF16),
            pltpu.VMEM((Y_FIRST, lanes_y, TILES, ROWS * CLASSES, BX, BZ), BF16),
            pltpu.VMEM((Y_FIRST, sides, lanes_y, TILES, CLASSES, BX, BZ), BF16),
            pltpu.VMEM((Y_FIRST, lanes_x, ROWS, DIFFS, BX, BZ), F32),
            pltpu.VMEM((Y_FIRST, lanes_x, ROWS, DIFFS, BX, BZ), F32),
            pltpu.VMEM((Y_FIRST, lanes_x // 2, ROWS, DIFFS, BX, BZ), F32),
            pltpu.VMEM((lanes_x, lanes_y * BY, BZ), F32),
            pltpu.VMEM((lanes_x, BX, BZ), F32),
            pltpu.VMEM((sides, lanes_x, BX, BZ), F32),
            pltpu.VMEM((lanes_y, BY, BZ), F32),
            pltpu.VMEM((lanes_y, lanes_x, BX, BZ), F32),
            pltpu.VMEM((sides, lanes_y, lanes_x, BX, BZ), F32),
            pltpu.VMEM((BY, BX, BZ), F32),
            dma((2,)),
            dma((PY // STEP,)),
            *[dma((X_FIRST,))] * 6,
            *[dma((Y_FIRST,))] * 5,
            dma((Y_FIRST, lanes_x)),
            dma((Y_FIRST,)),
            dma((Y_FIRST, lanes_x // 2)),
            *[pltpu.VMEM((lanes_x, MAIN, BX, BZ), BF16)] * X_FIRST,
        ],
        compiler_params=pltpu.CompilerParams(collective_id=0, has_side_effects=True),
    )(
        jnp.transpose(patch_start, (0, 3, 2, 1)),
        jnp.transpose(patch_owner, (0, 2, 1)),
        patch_logits[0, 0, 0],
    )
    return jnp.transpose(probs, (2, 0, 1, 3))


def solution(mesh):
    return jax.shard_map(
        per_device,
        mesh=mesh,
        in_specs=(P("gx", "gy", "gz", None, None), P(), P()),
        out_specs=P("gx", "gy", None, "gz"),
        check_vma=False,
    )
```
